32 devices in a mesh: lat: 16 (over z, y, x), lev: 2 (over core).
Axes of the slice: x: 2, y: 2, z: 4, core: 2. Of those that a mesh axis runs over, the one named last changes fastest.
Arguments:
- fields: float32 [160, 3, 16, 2560], P('lat', None, 'lev'), may hold values from 0.1 to 5
- lat_fraction: float32 [160], P('lat'), may hold values from 0 to 1
- lon_fraction: float32 [160], P('lat'), may hold values from 0 to 1
- lon_shift: int32 [160], P('lat'), may hold values from 0 to 2559
- departure_row: int32 [160], P('lat'), may hold values from 1 to 157, as said below
- extents: int32 [16, 2], P('lat'), may hold values from 1 to 4
Outputs:
- advected: float32 [160, 3, 16, 2560], P('lat', None, 'lev')
The draws below stay inside these ranges and needn't reach their ends.
Inputs may be any that keep to these rules, and one draw needn't show every extreme that they name: departure_row[r] lies within 39 rows of r.
All inputs are finite; a program needn't handle non-finite values.
Results may differ from the reference program's by a relative error of at most 0.0003.
Values sent between devices are 32-bit elements; how exact they have to be, the bound alone decides.
A program may use at most 128 MiB of HBM per device.

```python
import math
import jax
import jax.numpy as jnp
from jax import lax

ROWS = 10
LON = 2560
FIELDS = 3
REACH = 4
NLAT = 160
LEV = 16
BANDS = 16


def band_phase(key):
    return jax.random.randint(jax.random.fold_in(key, 911), (), 0, 8 * ROWS)


def draw_fields(key, part):
    row_phase = band_phase(key)
    shifted_rows = (jnp.arange(NLAT, dtype=jnp.int32) + row_phase) % (8 * ROWS)
    row_angle = 2.0 * math.pi * shifted_rows.astype(jnp.float32) / (8 * ROWS)
    full_shape = (NLAT, FIELDS, LEV, LON)
    gain_row = jnp.exp(-0.5 * jnp.sin(row_angle))
    rough_part = jax.random.uniform(jax.random.fold_in(key, 23), full_shape, jnp.float32, 0.5, 2.0)
    return (gain_row[:, None, None, None] * rough_part).astype(jnp.float32)


def draw_departure_row(key, part):
    row_phase = band_phase(key)
    row_ids = jnp.arange(NLAT, dtype=jnp.int32)
    shifted_rows = (row_ids + row_phase) % (8 * ROWS)
    row_drift = jnp.clip(2 * (2 * ROWS - jnp.abs(shifted_rows - 4 * ROWS)), -2 * ROWS, 2 * ROWS)
    row_noise = jax.random.randint(jax.random.fold_in(key, 17), (NLAT,), -2 * ROWS, 2 * ROWS + 1)
    offsets = jnp.clip(row_drift + row_noise, -REACH * ROWS + 1, REACH * ROWS - 2)
    spread = jax.random.randint(jax.random.fold_in(key, 29), (NLAT,), 0, 1 << 20)
    north_offset = -(1 + spread % (REACH * ROWS - 1))
    south_offset = 1 + spread % (REACH * ROWS - 2)
    position = row_ids % ROWS
    offsets = jnp.where(position == 0, north_offset, offsets)
    offsets = jnp.where(position == ROWS - 1, south_offset, offsets)
    return jnp.clip(row_ids + offsets, 1, NLAT - 3).astype(jnp.int32)


def plant(array, rng, low, largest):
    spot = [jax.random.randint(jax.random.fold_in(rng, axis), (), 0, length) for axis, length in enumerate(array.shape)]
    widest = array.shape.index(max(array.shape))
    next_to = spot[:widest] + [(spot[widest] + 1) % array.shape[widest]] + spot[widest + 1:]
    return array.at[tuple(spot)].set(low).at[tuple(next_to)].set(largest)


def level_of(stream_key, shape, pieces, smallest, high):
    def one(axis_at, blocks):
        heights = jax.random.uniform(jax.random.fold_in(jax.random.fold_in(stream_key, 6), axis_at), (blocks,), jnp.float32, smallest / len(pieces), high / len(pieces))
        return jnp.repeat(jnp.exp(heights), shape[axis_at] // blocks).reshape((-1,) + (1,) * (len(shape) - axis_at - 1))

    gain = one(*pieces[0])
    for cut in pieces[1:]:
        gain = gain * one(*cut)
    return gain


def setup_inputs(seed: int = 0) -> dict:
    key_of = jax.random.split(jax.random.key(seed), 7)
    return {
        "fields": draw_fields(jax.random.fold_in(key_of[6], 71), 0),
        "lat_fraction": jnp.clip(1.0 * jax.random.uniform(key_of[1], (NLAT,), jnp.float32) ** level_of(key_of[1], (NLAT,), ((0, 16),), -0.2, 0.2), 0.0, 1.0),
        "lon_fraction": jnp.clip(1.0 * jax.random.uniform(key_of[2], (NLAT,), jnp.float32) ** level_of(key_of[2], (NLAT,), ((0, 16),), -0.2, 0.2), 0.0, 1.0),
        "lon_shift": plant(jax.random.randint(key_of[3], (NLAT,), 0, LON), jax.random.fold_in(key_of[3], 1), 0, LON - 1).astype(jnp.int32),
        "departure_row": draw_departure_row(jax.random.fold_in(key_of[6], 71), 0),
        "extents": plant(jax.random.randint(key_of[5], (BANDS, 2), 1, REACH + 1), jax.random.fold_in(key_of[5], 1), 1, REACH).astype(jnp.int32),
    }


def cubic_weights(fraction):
    return jnp.stack([-fraction * (fraction - 1.0) * (fraction - 2.0) / 6.0,
                      (fraction + 1.0) * (fraction - 1.0) * (fraction - 2.0) / 2.0,
                      -(fraction + 1.0) * fraction * (fraction - 2.0) / 2.0,
                      (fraction + 1.0) * fraction * (fraction - 1.0) / 6.0])


def along_lon(column, lon_w, shift_value):
    lon_count = column.shape[-1]
    doubled = jnp.concatenate([column, column], axis=-1)
    result = jnp.zeros_like(column)
    for offset in range(4):
        first = ((shift_value + offset - 1) % lon_count).astype(jnp.int32)
        result = result + lon_w[offset] * lax.dynamic_slice_in_dim(doubled, first, lon_count, 2)
    return result


def reference(fields, lat_fraction, lon_fraction, lon_shift, departure_row, extents):
    row_ids = jnp.arange(NLAT, dtype=jnp.int32)
    band_ids = row_ids // ROWS
    low_bound = band_ids * ROWS - extents[band_ids, 0] * ROWS + 1
    high_bound = band_ids * ROWS + ROWS - 3 + extents[band_ids, 1] * ROWS
    departure = jnp.clip(jnp.clip(departure_row, low_bound, high_bound), 1, NLAT - 3).astype(jnp.int32)

    def one_row(inputs):
        dep_value, lat_t, lon_t, shift_value = inputs
        row_block = lax.dynamic_slice_in_dim(fields, (dep_value - 1).astype(jnp.int32), 4, 0)
        lat_w = cubic_weights(lat_t)
        column = lat_w[0] * row_block[0] + lat_w[1] * row_block[1] + lat_w[2] * row_block[2] + lat_w[3] * row_block[3]
        return along_lon(column, cubic_weights(lon_t), shift_value)

    moved = lax.map(one_row, (departure, lat_fraction, lon_fraction, lon_shift))
    area = jnp.cos(math.pi * (row_ids.astype(jnp.float32) + 0.5) / NLAT - math.pi / 2.0)
    mass_before = jnp.sum(area[:, None, None, None] * fields, axis=(0, 2, 3))
    mass_after = jnp.sum(area[:, None, None, None] * moved, axis=(0, 2, 3))
    return moved * (mass_before / mass_after)[None, :, None, None]
```

```python
import functools
import math

import jax
import jax.numpy as jnp
from jax import lax
from jax.experimental import pallas as pl
from jax.experimental.pallas import tpu as pltpu
from jax.sharding import PartitionSpec as P

REACH = 4
LANES = 128
DEPTH = 3
MESH = pl.DeviceIdType.MESH

UP = {
    0: [],
    1: [(0, 1), (0, 2), (0, 0)],
    2: [(0, 0), (0, 1), (0, 2), (1, 0)],
    3: [(1, 1), (1, 2), (1, 0), (0, 0)],
}
UP_OVER_ONE = {3: [(2, 0), (2, 1), (2, 2)], 2: [(1, 1), (1, 2)]}
UP_OVER_TWO = {3: [(0, 1), (0, 2)]}


def arrivals(member):
    def both(table):
        up = [(1, m, h) for m, h in table.get(member, [])]
        down = [(-1, 3 - m, h) for m, h in table.get(3 - member, [])]
        return up + down

    one = [(0, member ^ 1, h) for h in range(3)] + [(0, member ^ 3, 0)] + both(UP_OVER_ONE)
    two = [(0, member ^ 2, h) for h in range(3)] + [(0, member ^ 3, h) for h in (1, 2)] + both(UP_OVER_TWO)
    up = [(1, member, h) for h in range(3)] + [(1, m, h) for m, h in UP[member]]
    down = [(-1, member, h) for h in range(3)] + [(-1, 3 - m, h) for m, h in UP[3 - member]]
    return {"one": one, "two": two, "up": up, "down": down}


LINKS = ("one", "two", "up", "down")


def exchange_kernel(bands, fields_ref, halo_ref, send_sem, recv_sem):
    band = lax.axis_index("lat")
    group, position = band // 4, lax.rem(band, 4)
    has_up = group < bands // 4 - 1
    has_down = group > 0
    rows, field_count = fields_ref.shape[:2]

    def cut(part):
        first = field_count * part // 3
        return pl.ds(first, field_count * (part + 1) // 3 - first)

    def slot_of(distance):
        return distance + 4 if distance < 0 else distance + 3

    def halo_part(distance, part):
        return halo_ref.at[pl.ds(slot_of(distance) * rows, rows), cut(part)]

    def when(offset, body):
        if offset == 0:
            body()
        else:
            pl.when(has_up if offset == 1 else has_down)(body)

    barrier = pltpu.get_barrier_semaphore()

    def greet(step, condition):
        def body():
            pl.semaphore_signal(barrier, inc=1, device_id={"lat": band + step}, device_id_type=MESH)

        pl.when(condition)(body)

    even, low = lax.rem(position, 2) == 0, position < 2
    greet(1, even)
    greet(-1, jnp.logical_not(even))
    greet(2, low)
    greet(-2, jnp.logical_not(low))
    greet(4, has_up)
    greet(-4, has_down)
    pl.semaphore_wait(barrier, 2 + has_up.astype(jnp.int32) + has_down.astype(jnp.int32))

    for member in range(4):

        def run(member=member):
            incoming = arrivals(member)
            came_over = {item: (link, k) for link in LINKS for k, item in enumerate(incoming[link])}
            waited = set()

            def wait_for(item):
                if item in waited:
                    return
                waited.add(item)
                offset, m, h = item
                link, k = came_over[item]
                place = halo_part(4 * offset + m - member, h)

                def body():
                    pltpu.make_async_remote_copy(
                        src_ref=place, dst_ref=place,
                        send_sem=send_sem.at[LINKS.index(link), k],
                        recv_sem=recv_sem.at[LINKS.index(link), k],
                        device_id={"lat": band}, device_id_type=MESH,
                    ).wait_recv()

                when(offset, body)

            targets = [
                ("up", member, -4, -1),
                ("down", member, 4, 1),
                ("one", member ^ 1, (member ^ 1) - member, 0),
                ("two", member ^ 2, (member ^ 2) - member, 0),
            ]
            lists = [arrivals(target)[link] for link, target, _, _ in targets]
            sends = []
            for k in range(max(len(one) for one in lists)):
                for (link, target, step, group_step), items in zip(targets, lists):
                    if k >= len(items):
                        continue
                    offset, m, h = items[k]
                    here = offset + group_step
                    mine = here == 0 and m == member
                    if not mine:
                        wait_for((here, m, h))
                    source = fields_ref.at[:, cut(h)] if mine else halo_part(4 * here + m - member, h)
                    copy = pltpu.make_async_remote_copy(
                        src_ref=source,
                        dst_ref=halo_part(4 * offset + m - target, h),
                        send_sem=send_sem.at[LINKS.index(link), k],
                        recv_sem=recv_sem.at[LINKS.index(link), k],
                        device_id={"lat": band + step}, device_id_type=MESH,
                    )
                    condition = group_step if group_step else here
                    when(condition, copy.start)
                    sends.append((condition, copy))
            for k in range(max(len(incoming[link]) for link in LINKS)):
                for link in LINKS:
                    if k < len(incoming[link]):
                        wait_for(incoming[link][k])
            for condition, copy in sends:
                when(condition, copy.wait_send)

        pl.when(position == member)(run)


def exchange(fields):
    bands = lax.axis_size("lat")
    rows = fields.shape[0]
    if bands % 4 or fields.shape[1] < 3:
        blocks = []
        for distance in list(range(-REACH, 0)) + list(range(1, REACH + 1)):
            route = [(i + distance, i) for i in range(bands) if 0 <= i + distance < bands]
            blocks.append(lax.ppermute(fields, "lat", route))
        return jnp.concatenate(blocks, axis=0)
    return pl.pallas_call(
        functools.partial(exchange_kernel, bands),
        out_shape=jax.ShapeDtypeStruct((2 * REACH * rows,) + fields.shape[1:], fields.dtype),
        in_specs=[pl.BlockSpec(memory_space=pl.ANY)],
        out_specs=pl.BlockSpec(memory_space=pl.ANY),
        scratch_shapes=[pltpu.SemaphoreType.DMA((4, 7)), pltpu.SemaphoreType.DMA((4, 7))],
        compiler_params=pltpu.CompilerParams(collective_id=0, has_side_effects=True),
        cost_estimate=pl.CostEstimate(flops=0, bytes_accessed=16 * fields.size * 4 * 10, transcendentals=0),
        name="exchange",
    )(fields)


def row_kernel(start_ref, shift_ref, lat_w_ref, lon_w_ref, table_ref, area_ref, fields_ref, halo_ref, out_ref,
               held, doubled, ratio, sem):
    row = pl.program_id(0)
    row_count = pl.num_programs(0)
    rows, field_count, _, lon_count = fields_ref.shape
    tiles = lon_count // LANES

    def fetch(index):
        slot = lax.rem(index, DEPTH)
        for a in range(4):
            place = start_ref[index] + a
            own = jnp.logical_and(place >= REACH * rows, place < (REACH + 1) * rows)
            target = held.at[slot, a]

            @pl.when(own)
            def _():
                pltpu.make_async_copy(fields_ref.at[place - REACH * rows], target, sem.at[slot, a]).start()

            @pl.when(jnp.logical_not(own))
            def _():
                away = jnp.where(place < REACH * rows, place, place - rows)
                pltpu.make_async_copy(halo_ref.at[away], target, sem.at[slot, a]).start()

    @pl.when(row == 0)
    def _():
        for index in range(min(DEPTH - 1, rows)):
            fetch(index)
        weight = table_ref[field_count:field_count + 1, :]
        for f in range(field_count):
            total = table_ref[f:f + 1, :]
            before = jnp.sum(total * area_ref[...], axis=1, keepdims=True)
            after = jnp.sum(total * weight, axis=1, keepdims=True)
            ratio[f] = jnp.broadcast_to(before / after, ratio.shape[1:])

    @pl.when(row + DEPTH - 1 < row_count)
    def _():
        fetch(row + DEPTH - 1)

    slot = lax.rem(row, DEPTH)
    for a in range(4):
        pltpu.make_async_copy(fields_ref.at[0], held.at[slot, a], sem.at[slot, a]).wait()
    lane = lax.broadcasted_iota(jnp.int32, (out_ref.shape[2], LANES), 1)
    for f in range(field_count):
        column = lat_w_ref[row, 0] * held[slot, 0, f]
        for a in range(1, 4):
            column = column + lat_w_ref[row, a] * held[slot, a, f]
        doubled[f, :, 0:lon_count] = column
        doubled[f, :, lon_count:2 * lon_count] = column
        sums = [None] * tiles
        for k in range(4):
            first = lax.rem(shift_ref[row] + k - 1 + lon_count, lon_count)
            whole, rest = first // LANES, lax.rem(first, LANES)
            turn = lax.rem(LANES - rest, LANES)
            keep = lane < LANES - rest
            weight = lon_w_ref[row, k] * ratio[f]
            turned = []
            for t in range(tiles + 1):
                at = pl.multiple_of((whole + t) * LANES, LANES)
                turned.append(pltpu.roll(doubled[f, :, pl.ds(at, LANES)], turn, 1))
            for t in range(tiles):
                term = weight * jnp.where(keep, turned[t], turned[t + 1])
                sums[t] = term if sums[t] is None else sums[t] + term
        for t in range(tiles):
            out_ref[0, f, :, t * LANES:(t + 1) * LANES] = sums[t]


def rows_of(start, shift, lat_w, lon_w, table, area, fields, halo):
    rows, field_count, levels, lon_count = fields.shape
    smem = pl.BlockSpec(memory_space=pltpu.SMEM)
    return pl.pallas_call(
        row_kernel,
        grid=(rows,),
        out_shape=jax.ShapeDtypeStruct(fields.shape, fields.dtype),
        in_specs=[smem] * 4 + [pl.BlockSpec(memory_space=pltpu.VMEM)] * 2 + [pl.BlockSpec(memory_space=pl.ANY)] * 2,
        out_specs=pl.BlockSpec((1, field_count, levels, lon_count), lambda r: (r, 0, 0, 0)),
        scratch_shapes=[
            pltpu.VMEM((DEPTH, 4, field_count, levels, lon_count), jnp.float32),
            pltpu.VMEM((field_count, levels, 2 * lon_count), jnp.float32),
            pltpu.VMEM((field_count, levels, LANES), jnp.float32),
            pltpu.SemaphoreType.DMA((DEPTH, 4)),
        ],
        compiler_params=pltpu.CompilerParams(dimension_semantics=("arbitrary",)),
        name="rows",
    )(start, shift, lat_w, lon_w, table, area, fields, halo)


def cubic_weights(fraction):
    return jnp.stack(
        [
            -fraction * (fraction - 1.0) * (fraction - 2.0) / 6.0,
            (fraction + 1.0) * (fraction - 1.0) * (fraction - 2.0) / 2.0,
            -(fraction + 1.0) * fraction * (fraction - 2.0) / 2.0,
            (fraction + 1.0) * fraction * (fraction - 1.0) / 6.0,
        ],
        axis=-1,
    )


def area_of(row_ids, total_rows):
    return jnp.cos(math.pi * (row_ids.astype(jnp.float32) + 0.5) / total_rows - math.pi / 2.0)


def per_device(fields, lat_fraction, lon_fraction, lon_shift, departure_row, extents):
    rows = fields.shape[0]
    total_rows = lax.axis_size("lat") * rows
    first_row = lax.axis_index("lat") * rows
    low_bound = first_row - extents[0, 0] * rows + 1
    high_bound = first_row + rows - 3 + extents[0, 1] * rows
    departure = jnp.clip(jnp.clip(departure_row, low_bound, high_bound), 1, total_rows - 3)
    start = departure - 1 - (first_row - REACH * rows)
    lat_w, lon_w = cubic_weights(lat_fraction), cubic_weights(lon_fraction)

    row_area = area_of(first_row + jnp.arange(rows, dtype=jnp.int32), total_rows)
    share = (row_area * jnp.sum(lon_w, axis=1))[:, None] * lat_w / lax.axis_size("lev")
    all_rows = jnp.arange(total_rows, dtype=jnp.int32)
    reads = (departure - 1)[:, None] + jnp.arange(4, dtype=jnp.int32)[None, :]
    taken = jnp.sum(jnp.where(reads[:, :, None] == all_rows, share[:, :, None], 0.0), axis=(0, 1))
    sums = jnp.sum(fields, axis=(2, 3))
    mine = (first_row + jnp.arange(rows, dtype=jnp.int32))[:, None, None] == all_rows
    placed = jnp.sum(jnp.where(mine, sums[:, :, None], 0.0), axis=0)
    table = lax.psum(jnp.concatenate([placed, taken[None, :]], axis=0), ("lat", "lev"))

    halo = exchange(fields)
    return rows_of(start, lon_shift, lat_w, lon_w, table, area_of(all_rows, total_rows)[None, :], fields, halo)


def solution(mesh):
    return jax.shard_map(
        per_device,
        mesh=mesh,
        in_specs=(
            P("lat", None, "lev", None),
            P("lat"),
            P("lat"),
            P("lat"),
            P("lat"),
            P("lat", None),
        ),
        out_specs=P("lat", None, "lev", None),
        check_vma=False,
    )
```

```python
import functools
import math

import jax
import jax.numpy as jnp
import numpy as np
from jax import lax
from jax.experimental import pallas as pl
from jax.experimental.pallas import tpu as pltpu
from jax.sharding import PartitionSpec as P

REACH = 4
LANES = 128
DEPTH = 3
MESH = pl.DeviceIdType.MESH

UP = {
    0: [],
    1: [(0, 1), (0, 2), (0, 0)],
    2: [(0, 0), (0, 1), (0, 2), (1, 0)],
    3: [(1, 1), (1, 2), (1, 0), (0, 0)],
}
UP_OVER_ONE = {3: [(2, 0), (2, 1), (2, 2)], 2: [(1, 1), (1, 2)]}
UP_OVER_TWO = {3: [(0, 1), (0, 2)]}


def arrivals(member):
    def both(table):
        up = [(1, m, h) for m, h in table.get(member, [])]
        down = [(-1, 3 - m, h) for m, h in table.get(3 - member, [])]
        return up + down

    one = [(0, member ^ 1, h) for h in range(3)] + [(0, member ^ 3, 0)] + both(UP_OVER_ONE)
    two = [(0, member ^ 2, h) for h in range(3)] + [(0, member ^ 3, h) for h in (1, 2)] + both(UP_OVER_TWO)
    up = [(1, member, h) for h in range(3)] + [(1, m, h) for m, h in UP[member]]
    down = [(-1, member, h) for h in range(3)] + [(-1, 3 - m, h) for m, h in UP[3 - member]]
    return {"one": one, "two": two, "up": up, "down": down}


LINKS = ("one", "two", "up", "down")


def cubic(t):
    sixth = 1.0 / 6.0
    return (
        -t * (t - 1.0) * (t - 2.0) * sixth,
        (t + 1.0) * (t - 1.0) * (t - 2.0) * 0.5,
        -(t + 1.0) * t * (t - 2.0) * 0.5,
        (t + 1.0) * t * (t - 1.0) * sixth,
    )


def departure_of(row, first_row, rows, total_rows, departure_ref, extents_ref):
    low = first_row - extents_ref[0, 0] * rows + 1
    high = first_row + rows - 3 + extents_ref[0, 1] * rows
    inside = jnp.minimum(jnp.maximum(departure_ref[row], low), high)
    return jnp.minimum(jnp.maximum(inside, 1), total_rows - 3)


def exchange_kernel(bands, levs, lat_t_ref, lon_t_ref, departure_ref, extents_ref, area_ref, fields_ref,
                    halo_ref, table_ref, held, mine, met, sent, gathered, send_sem, recv_sem, local_sem,
                    table_send_sem, table_recv_sem):
    band, lev = lax.axis_index("lat"), lax.axis_index("lev")
    group, position = band // 4, lax.rem(band, 4)
    groups = bands // 4
    has_up = group < groups - 1
    has_down = group > 0
    rows, field_count = fields_ref.shape[:2]
    first_row, total_rows = band * rows, bands * rows
    step_one = 1 - 2 * lax.rem(position, 2)
    step_two = 2 - 4 * (position // 2)
    across = [{"lev": 1 - lev}, {"lat": band + step_one}, {"lat": band + step_two}]
    others = [{"lat": lax.rem(band + 4 * j, bands)} for j in range(1, groups)]

    barrier = pltpu.get_barrier_semaphore()
    for peer in across + others:
        pl.semaphore_signal(barrier, inc=1, device_id=peer, device_id_type=MESH)
    pl.semaphore_wait(barrier, len(across) + len(others))

    def cut(part):
        first = field_count * part // 3
        return pl.ds(first, field_count * (part + 1) // 3 - first)

    def halo_part(distance, part):
        slot = distance + 4 if distance < 0 else distance + 3
        return halo_ref.at[pl.ds(slot * rows, rows), cut(part)]

    def when(offset, body):
        if offset == 0:
            body()
        else:
            pl.when(has_up if offset == 1 else has_down)(body)

    came_over = [
        {item: (link, k) for link, items in arrivals(member).items() for k, item in enumerate(items)}
        for member in range(4)
    ]
    waited = [set() for _ in range(4)]

    def wait_for(member, item):
        if item in waited[member]:
            return
        waited[member].add(item)
        offset, m, h = item
        link, k = came_over[member][item]
        place = halo_part(4 * offset + m - member, h)
        when(
            offset,
            lambda: pltpu.make_async_remote_copy(
                src_ref=place, dst_ref=place,
                send_sem=send_sem.at[LINKS.index(link), k],
                recv_sem=recv_sem.at[LINKS.index(link), k],
                device_id={"lat": band}, device_id_type=MESH,
            ).wait_recv(),
        )

    def targets(member):
        return [
            ("up", member, -4, -1),
            ("down", member, 4, 1),
            ("one", member ^ 1, (member ^ 1) - member, 0),
            ("two", member ^ 2, (member ^ 2) - member, 0),
        ]

    def sends(member, k):
        for link, target, step, group_step in targets(member):
            items = arrivals(target)[link]
            if k < len(items):
                offset, m, h = items[k]
                here = offset + group_step
                own = here == 0 and m == member
                copy = pltpu.make_async_remote_copy(
                    src_ref=fields_ref.at[:, cut(h)] if own else halo_part(4 * here + m - member, h),
                    dst_ref=halo_part(4 * offset + m - target, h),
                    send_sem=send_sem.at[LINKS.index(link), k],
                    recv_sem=recv_sem.at[LINKS.index(link), k],
                    device_id={"lat": band + step}, device_id_type=MESH,
                )
                yield (None if own else (here, m, h)), (group_step if group_step else here), copy

    def on_each(body):
        for member in range(4):
            pl.when(position == member)(functools.partial(body, member))

    def send_pieces(*steps):
        def body(member):
            for k in steps:
                for item, condition, copy in sends(member, k):
                    if item is not None:
                        wait_for(member, item)
                    when(condition, copy.start)

        on_each(body)

    def table_copy(n, source, target, peer):
        return pltpu.make_async_remote_copy(
            src_ref=source, dst_ref=target, send_sem=table_send_sem.at[n], recv_sem=table_recv_sem.at[n],
            device_id=peer, device_id_type=MESH,
        )

    load = pltpu.make_async_copy(fields_ref, held, local_sem)
    load.start()
    send_pieces(0)

    lane = lax.broadcasted_iota(jnp.int32, (1, table_ref.shape[1]), 1)
    taken = jnp.zeros(lane.shape, jnp.float32)
    for row in range(rows):
        departure = departure_of(row, first_row, rows, total_rows, departure_ref, extents_ref)
        lon_w = cubic(lon_t_ref[row])
        share = area_ref[first_row + row] * (lon_w[0] + lon_w[1] + lon_w[2] + lon_w[3]) * (1.0 / levs)
        for a, weight in enumerate(cubic(lat_t_ref[row])):
            taken = taken + jnp.where(lane == departure - 1 + a, share * weight, 0.0)
    load.wait()
    sums = [jnp.zeros(lane.shape, jnp.float32) for _ in range(field_count)]
    for row in range(rows):
        for f in range(field_count):
            total = jnp.sum(jnp.sum(held[row, f], axis=0, keepdims=True), axis=1, keepdims=True)
            sums[f] = sums[f] + jnp.where(lane == first_row + row, total, 0.0)
    mine[...] = jnp.zeros_like(mine)
    for f in range(field_count):
        mine[f:f + 1, :] = sums[f]
    mine[field_count:field_count + 1, :] = taken

    def table_step(n):
        return table_copy(n, mine if n == 0 else sent.at[n - 1], met.at[n], across[n])

    def table_add(n):
        table_step(n).wait_recv()
        sent[n] = (mine[...] if n == 0 else sent[n - 1]) + met[n]

    table_step(0).start()
    table_add(0)
    table_step(1).start()
    send_pieces(1, 2)
    table_add(1)
    table_step(2).start()
    send_pieces(3, 4)
    table_add(2)
    last = [table_copy(3 + j, sent.at[2], gathered.at[j], peer) for j, peer in enumerate(others)]
    for copy in last:
        copy.start()
    send_pieces(5, 6)
    for copy in last:
        copy.wait_recv()
    result = sent[2]
    for j in range(len(others)):
        result = result + gathered[j]
    table_ref[...] = result

    def finish(member):
        for k in range(7):
            for link in LINKS:
                items = arrivals(member)[link]
                if k < len(items):
                    wait_for(member, items[k])
        for k in range(7):
            for _, condition, copy in sends(member, k):
                when(condition, copy.wait_send)

    on_each(finish)
    for n in range(3):
        table_step(n).wait_send()
    for copy in last:
        copy.wait_send()


def exchange(lat_t, lon_t, departure_row, extents, area, fields):
    bands, levs = lax.axis_size("lat"), lax.axis_size("lev")
    rows, field_count = fields.shape[:2]
    table = ((field_count + 8) // 8 * 8, -(-bands * rows // LANES) * LANES)
    others = bands // 4 - 1
    return pl.pallas_call(
        functools.partial(exchange_kernel, bands, levs),
        out_shape=(
            jax.ShapeDtypeStruct((2 * REACH * rows,) + fields.shape[1:], fields.dtype),
            jax.ShapeDtypeStruct(table, jnp.float32),
        ),
        in_specs=[pl.BlockSpec(memory_space=pltpu.SMEM)] * 5 + [pl.BlockSpec(memory_space=pl.ANY)],
        out_specs=(pl.BlockSpec(memory_space=pl.ANY), pl.BlockSpec(memory_space=pltpu.VMEM)),
        scratch_shapes=[
            pltpu.VMEM(fields.shape, jnp.float32),
            pltpu.VMEM(table, jnp.float32),
            pltpu.VMEM((3,) + table, jnp.float32),
            pltpu.VMEM((3,) + table, jnp.float32),
            pltpu.VMEM((max(others, 1),) + table, jnp.float32),
            pltpu.SemaphoreType.DMA((4, 7)),
            pltpu.SemaphoreType.DMA((4, 7)),
            pltpu.SemaphoreType.DMA,
            pltpu.SemaphoreType.DMA((3 + others,)),
            pltpu.SemaphoreType.DMA((3 + others,)),
        ],
        compiler_params=pltpu.CompilerParams(collective_id=0, has_side_effects=True),
        name="exchange",
    )(lat_t, lon_t, departure_row, extents, area, fields)


def row_kernel(bands, lat_t_ref, lon_t_ref, shift_ref, departure_ref, extents_ref, table_ref, area_ref, fields_ref,
               halo_ref, out_ref, held, doubled, ratio, sem):
    row = pl.program_id(0)
    row_count = pl.num_programs(0)
    rows, field_count, _, lon_count = fields_ref.shape
    tiles = lon_count // LANES
    first_row = lax.axis_index("lat") * rows

    def fetch(index):
        slot = lax.rem(index, DEPTH)
        departure = departure_of(index, first_row, rows, bands * rows, departure_ref, extents_ref)
        start = departure - 1 - (first_row - REACH * rows)
        for a in range(4):
            place = start + a
            own = jnp.logical_and(place >= REACH * rows, place < (REACH + 1) * rows)
            target = held.at[slot, a]

            @pl.when(own)
            def _():
                pltpu.make_async_copy(fields_ref.at[place - REACH * rows], target, sem.at[slot, a]).start()

            @pl.when(jnp.logical_not(own))
            def _():
                away = jnp.where(place < REACH * rows, place, place - rows)
                pltpu.make_async_copy(halo_ref.at[away], target, sem.at[slot, a]).start()

    @pl.when(row == 0)
    def _():
        for index in range(min(DEPTH - 1, rows)):
            fetch(index)
        weight = table_ref[field_count:field_count + 1, :]
        for f in range(field_count):
            total = table_ref[f:f + 1, :]
            before = jnp.sum(total * area_ref[...], axis=1, keepdims=True)
            after = jnp.sum(total * weight, axis=1, keepdims=True)
            ratio[f] = jnp.broadcast_to(before / after, ratio.shape[1:])

    @pl.when(row + DEPTH - 1 < row_count)
    def _():
        fetch(row + DEPTH - 1)

    slot = lax.rem(row, DEPTH)
    for a in range(4):
        pltpu.make_async_copy(fields_ref.at[0], held.at[slot, a], sem.at[slot, a]).wait()
    lat_w, lon_w = cubic(lat_t_ref[row]), cubic(lon_t_ref[row])
    lane = lax.broadcasted_iota(jnp.int32, (out_ref.shape[2], LANES), 1)
    for f in range(field_count):
        column = lat_w[0] * held[slot, 0, f]
        for a in range(1, 4):
            column = column + lat_w[a] * held[slot, a, f]
        doubled[f, :, 0:lon_count] = column
        doubled[f, :, lon_count:2 * lon_count] = column
        sums = [None] * tiles
        for k in range(4):
            first = lax.rem(shift_ref[row] + k - 1 + lon_count, lon_count)
            whole, rest = first // LANES, lax.rem(first, LANES)
            turn = lax.rem(LANES - rest, LANES)
            keep = lane < LANES - rest
            weight = lon_w[k] * ratio[f]
            turned = []
            for t in range(tiles + 1):
                at = pl.multiple_of((whole + t) * LANES, LANES)
                turned.append(pltpu.roll(doubled[f, :, pl.ds(at, LANES)], turn, 1))
            for t in range(tiles):
                term = weight * jnp.where(keep, turned[t], turned[t + 1])
                sums[t] = term if sums[t] is None else sums[t] + term
        for t in range(tiles):
            out_ref[0, f, :, t * LANES:(t + 1) * LANES] = sums[t]


def rows_of(bands, lat_t, lon_t, shift, departure_row, extents, table, area, fields, halo):
    rows, field_count, levels, lon_count = fields.shape
    smem = pl.BlockSpec(memory_space=pltpu.SMEM)
    return pl.pallas_call(
        functools.partial(row_kernel, bands),
        grid=(rows,),
        out_shape=jax.ShapeDtypeStruct(fields.shape, fields.dtype),
        in_specs=[smem] * 5 + [pl.BlockSpec(memory_space=pltpu.VMEM)] * 2 + [pl.BlockSpec(memory_space=pl.ANY)] * 2,
        out_specs=pl.BlockSpec((1, field_count, levels, lon_count), lambda r: (r, 0, 0, 0)),
        scratch_shapes=[
            pltpu.VMEM((DEPTH, 4, field_count, levels, lon_count), jnp.float32),
            pltpu.VMEM((field_count, levels, 2 * lon_count), jnp.float32),
            pltpu.VMEM((field_count, levels, LANES), jnp.float32),
            pltpu.SemaphoreType.DMA((DEPTH, 4)),
        ],
        compiler_params=pltpu.CompilerParams(dimension_semantics=("arbitrary",)),
        name="rows",
    )(lat_t, lon_t, shift, departure_row, extents, table, area, fields, halo)


def per_device(fields, lat_fraction, lon_fraction, lon_shift, departure_row, extents):
    bands = lax.axis_size("lat")
    total_rows = bands * fields.shape[0]
    row_ids = np.arange(-(-total_rows // LANES) * LANES)
    area = np.where(row_ids < total_rows, np.cos(math.pi * (row_ids + 0.5) / total_rows - math.pi / 2.0), 0.0)
    area = jnp.asarray(area, jnp.float32)
    halo, table = exchange(lat_fraction, lon_fraction, departure_row, extents, area, fields)
    return rows_of(
        bands, lat_fraction, lon_fraction, lon_shift, departure_row, extents, table, area[None, :], fields, halo
    )


def solution(mesh):
    return jax.shard_map(
        per_device,
        mesh=mesh,
        in_specs=(
            P("lat", None, "lev", None),
            P("lat"),
            P("lat"),
            P("lat"),
            P("lat"),
            P("lat", None),
        ),
        out_specs=P("lat", None, "lev", None),
        check_vma=False,
    )
```

```python
import functools
import math

import jax
import jax.numpy as jnp
import numpy as np
from jax import lax
from jax.experimental import pallas as pl
from jax.experimental.pallas import tpu as pltpu
from jax.sharding import PartitionSpec as P

REACH = 4
LANES = 128
DEPTH = 10
MESH = pl.DeviceIdType.MESH

UP = {
    0: [],
    1: [(0, 1), (0, 2), (0, 0)],
    2: [(0, 0), (0, 1), (0, 2), (1, 0)],
    3: [(1, 1), (1, 2), (1, 0), (0, 0)],
}
UP_OVER_ONE = {3: [(2, 0), (2, 1), (2, 2)], 2: [(1, 1), (1, 2)]}
UP_OVER_TWO = {3: [(0, 1), (0, 2)]}


def arrivals(member):
    def both(table):
        up = [(1, m, h) for m, h in table.get(member, [])]
        down = [(-1, 3 - m, h) for m, h in table.get(3 - member, [])]
        return up + down

    one = [(0, member ^ 1, h) for h in range(3)] + [(0, member ^ 3, 0)] + both(UP_OVER_ONE)
    two = [(0, member ^ 2, h) for h in range(3)] + [(0, member ^ 3, h) for h in (1, 2)] + both(UP_OVER_TWO)
    up = [(1, member, h) for h in range(3)] + [(1, m, h) for m, h in UP[member]]
    down = [(-1, member, h) for h in range(3)] + [(-1, 3 - m, h) for m, h in UP[3 - member]]
    return {"one": one, "two": two, "up": up, "down": down}


LINKS = ("one", "two", "up", "down")


def cubic(t):
    sixth = 1.0 / 6.0
    return (
        -t * (t - 1.0) * (t - 2.0) * sixth,
        (t + 1.0) * (t - 1.0) * (t - 2.0) * 0.5,
        -(t + 1.0) * t * (t - 2.0) * 0.5,
        (t + 1.0) * t * (t - 1.0) * sixth,
    )


def departure_of(row, first_row, rows, total_rows, departure_ref, extents_ref):
    low = first_row - extents_ref[0, 0] * rows + 1
    high = first_row + rows - 3 + extents_ref[0, 1] * rows
    inside = jnp.minimum(jnp.maximum(departure_ref[row], low), high)
    return jnp.minimum(jnp.maximum(inside, 1), total_rows - 3)


def exchange_kernel(bands, levs, lat_t_ref, lon_t_ref, departure_ref, extents_ref, area_ref, fields_ref,
                    halo_ref, table_ref, held, mine, met, sent, gathered, send_sem, recv_sem, local_sem,
                    table_send_sem, table_recv_sem):
    band, lev = lax.axis_index("lat"), lax.axis_index("lev")
    group, position = band // 4, lax.rem(band, 4)
    groups = bands // 4
    has_up = group < groups - 1
    has_down = group > 0
    rows, field_count = fields_ref.shape[:2]
    first_row, total_rows = band * rows, bands * rows
    step_one = 1 - 2 * lax.rem(position, 2)
    step_two = 2 - 4 * (position // 2)
    across = [{"lev": 1 - lev}, {"lat": band + step_one}, {"lat": band + step_two}]
    others = [{"lat": lax.rem(band + 4 * j, bands)} for j in range(1, groups)]

    barrier = pltpu.get_barrier_semaphore()
    for peer in across + others:
        pl.semaphore_signal(barrier, inc=1, device_id=peer, device_id_type=MESH)
    pl.semaphore_wait(barrier, len(across) + len(others))

    def cut(part):
        first = field_count * part // 3
        return pl.ds(first, field_count * (part + 1) // 3 - first)

    def halo_part(distance, part):
        slot = distance + 4 if distance < 0 else distance + 3
        return halo_ref.at[pl.ds(slot * rows, rows), cut(part)]

    def when(offset, body):
        if offset == 0:
            body()
        else:
            pl.when(has_up if offset == 1 else has_down)(body)

    came_over = [
        {item: (link, k) for link, items in arrivals(member).items() for k, item in enumerate(items)}
        for member in range(4)
    ]
    waited = [set() for _ in range(4)]

    def wait_for(member, item):
        if item in waited[member]:
            return
        waited[member].add(item)
        offset, m, h = item
        link, k = came_over[member][item]
        place = halo_part(4 * offset + m - member, h)
        when(
            offset,
            lambda: pltpu.make_async_remote_copy(
                src_ref=place, dst_ref=place,
                send_sem=send_sem.at[LINKS.index(link), k],
                recv_sem=recv_sem.at[LINKS.index(link), k],
                device_id={"lat": band}, device_id_type=MESH,
            ).wait_recv(),
        )

    def targets(member):
        return [
            ("up", member, -4, -1),
            ("down", member, 4, 1),
            ("one", member ^ 1, (member ^ 1) - member, 0),
            ("two", member ^ 2, (member ^ 2) - member, 0),
        ]

    def sends(member, k):
        for link, target, step, group_step in targets(member):
            items = arrivals(target)[link]
            if k < len(items):
                offset, m, h = items[k]
                here = offset + group_step
                own = here == 0 and m == member
                copy = pltpu.make_async_remote_copy(
                    src_ref=fields_ref.at[:, cut(h)] if own else halo_part(4 * here + m - member, h),
                    dst_ref=halo_part(4 * offset + m - target, h),
                    send_sem=send_sem.at[LINKS.index(link), k],
                    recv_sem=recv_sem.at[LINKS.index(link), k],
                    device_id={"lat": band + step}, device_id_type=MESH,
                )
                yield (None if own else (here, m, h)), (group_step if group_step else here), copy

    def on_each(body):
        for member in range(4):
            pl.when(position == member)(functools.partial(body, member))

    def send_pieces(*steps):
        def body(member):
            for k in steps:
                for item, condition, copy in sends(member, k):
                    if item is not None:
                        wait_for(member, item)
                    when(condition, copy.start)

        on_each(body)

    def table_copy(n, source, target, peer):
        return pltpu.make_async_remote_copy(
            src_ref=source, dst_ref=target, send_sem=table_send_sem.at[n], recv_sem=table_recv_sem.at[n],
            device_id=peer, device_id_type=MESH,
        )

    load = pltpu.make_async_copy(fields_ref, held, local_sem)
    load.start()
    send_pieces(0)

    lane = lax.broadcasted_iota(jnp.int32, (1, table_ref.shape[1]), 1)
    taken = jnp.zeros(lane.shape, jnp.float32)
    for row in range(rows):
        departure = departure_of(row, first_row, rows, total_rows, departure_ref, extents_ref)
        lon_w = cubic(lon_t_ref[row])
        share = area_ref[first_row + row] * (lon_w[0] + lon_w[1] + lon_w[2] + lon_w[3]) * (1.0 / levs)
        for a, weight in enumerate(cubic(lat_t_ref[row])):
            taken = taken + jnp.where(lane == departure - 1 + a, share * weight, 0.0)
    load.wait()
    sums = [jnp.zeros(lane.shape, jnp.float32) for _ in range(field_count)]
    for row in range(rows):
        for f in range(field_count):
            total = jnp.sum(jnp.sum(held[row, f], axis=0, keepdims=True), axis=1, keepdims=True)
            sums[f] = sums[f] + jnp.where(lane == first_row + row, total, 0.0)
    mine[...] = jnp.zeros_like(mine)
    for f in range(field_count):
        mine[f:f + 1, :] = sums[f]
    mine[field_count:field_count + 1, :] = taken

    def table_step(n):
        return table_copy(n, mine if n == 0 else sent.at[n - 1], met.at[n], across[n])

    def table_add(n):
        table_step(n).wait_recv()
        sent[n] = (mine[...] if n == 0 else sent[n - 1]) + met[n]

    table_step(0).start()
    table_add(0)
    table_step(1).start()
    send_pieces(1, 2)
    table_add(1)
    table_step(2).start()
    send_pieces(3, 4)
    table_add(2)
    last = [table_copy(3 + j, sent.at[2], gathered.at[j], peer) for j, peer in enumerate(others)]
    for copy in last:
        copy.start()
    send_pieces(5, 6)
    for copy in last:
        copy.wait_recv()
    result = sent[2]
    for j in range(len(others)):
        result = result + gathered[j]
    table_ref[...] = result

    def finish(member):
        for k in range(7):
            for link in LINKS:
                items = arrivals(member)[link]
                if k < len(items):
                    wait_for(member, items[k])
        for k in range(7):
            for _, condition, copy in sends(member, k):
                when(condition, copy.wait_send)

    on_each(finish)
    for n in range(3):
        table_step(n).wait_send()
    for copy in last:
        copy.wait_send()


def exchange(lat_t, lon_t, departure_row, extents, area, fields):
    bands, levs = lax.axis_size("lat"), lax.axis_size("lev")
    rows, field_count = fields.shape[:2]
    table = ((field_count + 8) // 8 * 8, -(-bands * rows // LANES) * LANES)
    others = bands // 4 - 1
    return pl.pallas_call(
        functools.partial(exchange_kernel, bands, levs),
        out_shape=(
            jax.ShapeDtypeStruct((2 * REACH * rows,) + fields.shape[1:], fields.dtype),
            jax.ShapeDtypeStruct(table, jnp.float32),
        ),
        in_specs=[pl.BlockSpec(memory_space=pltpu.SMEM)] * 5 + [pl.BlockSpec(memory_space=pl.ANY)],
        out_specs=(pl.BlockSpec(memory_space=pl.ANY), pl.BlockSpec(memory_space=pltpu.VMEM)),
        scratch_shapes=[
            pltpu.VMEM(fields.shape, jnp.float32),
            pltpu.VMEM(table, jnp.float32),
            pltpu.VMEM((3,) + table, jnp.float32),
            pltpu.VMEM((3,) + table, jnp.float32),
            pltpu.VMEM((max(others, 1),) + table, jnp.float32),
            pltpu.SemaphoreType.DMA((4, 7)),
            pltpu.SemaphoreType.DMA((4, 7)),
            pltpu.SemaphoreType.DMA,
            pltpu.SemaphoreType.DMA((3 + others,)),
            pltpu.SemaphoreType.DMA((3 + others,)),
        ],
        compiler_params=pltpu.CompilerParams(collective_id=0, has_side_effects=True),
        name="exchange",
    )(lat_t, lon_t, departure_row, extents, area, fields)


def row_kernel(bands, lat_t_ref, lon_t_ref, shift_ref, departure_ref, extents_ref, table_ref, area_ref, fields_ref,
               halo_ref, out_ref, held, doubled, ratio, sem):
    row = pl.program_id(0)
    row_count = pl.num_programs(0)
    rows, field_count, _, lon_count = fields_ref.shape
    tiles = lon_count // LANES
    depth = held.shape[0]
    first_row = lax.axis_index("lat") * rows

    def fetch(index):
        slot = lax.rem(index, depth)
        departure = departure_of(index, first_row, rows, bands * rows, departure_ref, extents_ref)
        start = departure - 1 - (first_row - REACH * rows)
        for a in range(4):
            place = start + a
            own = jnp.logical_and(place >= REACH * rows, place < (REACH + 1) * rows)
            target = held.at[slot, a]

            @pl.when(own)
            def _():
                pltpu.make_async_copy(fields_ref.at[place - REACH * rows], target, sem.at[slot, a]).start()

            @pl.when(jnp.logical_not(own))
            def _():
                away = jnp.where(place < REACH * rows, place, place - rows)
                pltpu.make_async_copy(halo_ref.at[away], target, sem.at[slot, a]).start()

    @pl.when(row == 0)
    def _():
        for index in range(min(depth - 1, rows)):
            fetch(index)
        weight = table_ref[field_count:field_count + 1, :]
        for f in range(field_count):
            total = table_ref[f:f + 1, :]
            before = jnp.sum(total * area_ref[...], axis=1, keepdims=True)
            after = jnp.sum(total * weight, axis=1, keepdims=True)
            ratio[f] = jnp.broadcast_to(before / after, ratio.shape[1:])

    @pl.when(row + depth - 1 < row_count)
    def _():
        fetch(row + depth - 1)

    slot = lax.rem(row, depth)
    for a in range(4):
        pltpu.make_async_copy(fields_ref.at[0], held.at[slot, a], sem.at[slot, a]).wait()
    lat_w, lon_w = cubic(lat_t_ref[row]), cubic(lon_t_ref[row])
    lane = lax.broadcasted_iota(jnp.int32, (out_ref.shape[2], LANES), 1)
    first = lax.rem(shift_ref[row] - 1 + lon_count, lon_count)
    whole, rest = first // LANES, lax.rem(first, LANES)
    turn = lax.rem(LANES - rest, LANES)
    keep = lane < LANES - rest

    def ahead(pieces, step):
        turned = [pltpu.roll(piece, LANES - step, 1) for piece in pieces]
        return [jnp.where(lane < LANES - step, turned[t], turned[(t + 1) % tiles]) for t in range(tiles)]

    for f in range(field_count):
        lon = [weight * ratio[f] for weight in lon_w]
        column = []
        for t in range(tiles):
            at = pl.ds(t * LANES, LANES)
            total = lat_w[0] * held[slot, 0, f, :, at]
            for a in range(1, 4):
                total = total + lat_w[a] * held[slot, a, f, :, at]
            column.append(total)
        after = ahead(column, 1)
        later = ahead([lon[2] * column[t] + lon[3] * after[t] for t in range(tiles)], 2)
        for t in range(tiles):
            mixed = lon[0] * column[t] + lon[1] * after[t] + later[t]
            doubled[f, :, t * LANES:(t + 1) * LANES] = mixed
            doubled[f, :, lon_count + t * LANES:lon_count + (t + 1) * LANES] = mixed
        turned = []
        for t in range(tiles + 1):
            at = pl.multiple_of((whole + t) * LANES, LANES)
            turned.append(pltpu.roll(doubled[f, :, pl.ds(at, LANES)], turn, 1))
        for t in range(tiles):
            out_ref[0, f, :, t * LANES:(t + 1) * LANES] = jnp.where(keep, turned[t], turned[t + 1])


def rows_of(bands, lat_t, lon_t, shift, departure_row, extents, table, area, fields, halo):
    rows, field_count, levels, lon_count = fields.shape
    smem = pl.BlockSpec(memory_space=pltpu.SMEM)
    return pl.pallas_call(
        functools.partial(row_kernel, bands),
        grid=(rows,),
        out_shape=jax.ShapeDtypeStruct(fields.shape, fields.dtype),
        in_specs=[smem] * 5 + [pl.BlockSpec(memory_space=pltpu.VMEM)] * 2 + [pl.BlockSpec(memory_space=pl.ANY)] * 2,
        out_specs=pl.BlockSpec((1, field_count, levels, lon_count), lambda r: (r, 0, 0, 0)),
        scratch_shapes=[
            pltpu.VMEM((DEPTH, 4, field_count, levels, lon_count), jnp.float32),
            pltpu.VMEM((field_count, levels, 2 * lon_count), jnp.float32),
            pltpu.VMEM((field_count, levels, LANES), jnp.float32),
            pltpu.SemaphoreType.DMA((DEPTH, 4)),
        ],
        compiler_params=pltpu.CompilerParams(dimension_semantics=("arbitrary",)),
        name="rows",
    )(lat_t, lon_t, shift, departure_row, extents, table, area, fields, halo)


def per_device(fields, lat_fraction, lon_fraction, lon_shift, departure_row, extents):
    bands = lax.axis_size("lat")
    total_rows = bands * fields.shape[0]
    row_ids = np.arange(-(-total_rows // LANES) * LANES)
    area = np.where(row_ids < total_rows, np.cos(math.pi * (row_ids + 0.5) / total_rows - math.pi / 2.0), 0.0)
    area = jnp.asarray(area, jnp.float32)
    halo, table = exchange(lat_fraction, lon_fraction, departure_row, extents, area, fields)
    return rows_of(
        bands, lat_fraction, lon_fraction, lon_shift, departure_row, extents, table, area[None, :], fields, halo
    )


def solution(mesh):
    return jax.shard_map(
        per_device,
        mesh=mesh,
        in_specs=(
            P("lat", None, "lev", None),
            P("lat"),
            P("lat"),
            P("lat"),
            P("lat"),
            P("lat", None),
        ),
        out_specs=P("lat", None, "lev", None),
        check_vma=False,
    )
```

```python
import functools
import math

import jax
import jax.numpy as jnp
import numpy as np
from jax import lax
from jax.experimental import pallas as pl
from jax.experimental.pallas import tpu as pltpu
from jax.sharding import PartitionSpec as P

REACH = 4
LANES = 128
DEPTH = 5
MESH = pl.DeviceIdType.MESH

UP = {
    0: [],
    1: [(0, 1), (0, 2), (0, 0)],
    2: [(0, 0), (0, 1), (0, 2), (1, 0)],
    3: [(1, 1), (1, 2), (1, 0), (0, 0)],
}
UP_OVER_ONE = {3: [(2, 0), (2, 1), (2, 2)], 2: [(1, 1), (1, 2)]}
UP_OVER_TWO = {3: [(0, 1), (0, 2)]}


def arrivals(member):
    def both(table):
        up = [(1, m, h) for m, h in table.get(member, [])]
        down = [(-1, 3 - m, h) for m, h in table.get(3 - member, [])]
        return up + down

    one = [(0, member ^ 1, h) for h in range(3)] + [(0, member ^ 3, 0)] + both(UP_OVER_ONE)
    two = [(0, member ^ 2, h) for h in range(3)] + [(0, member ^ 3, h) for h in (1, 2)] + both(UP_OVER_TWO)
    up = [(1, member, h) for h in range(3)] + [(1, m, h) for m, h in UP[member]]
    down = [(-1, member, h) for h in range(3)] + [(-1, 3 - m, h) for m, h in UP[3 - member]]
    return {"one": one, "two": two, "up": up, "down": down}


LINKS = ("one", "two", "up", "down")


def cubic(t):
    sixth = 1.0 / 6.0
    return (
        -t * (t - 1.0) * (t - 2.0) * sixth,
        (t + 1.0) * (t - 1.0) * (t - 2.0) * 0.5,
        -(t + 1.0) * t * (t - 2.0) * 0.5,
        (t + 1.0) * t * (t - 1.0) * sixth,
    )


def departure_of(row, first_row, rows, total_rows, departure_ref, extents_ref):
    low = first_row - extents_ref[0, 0] * rows + 1
    high = first_row + rows - 3 + extents_ref[0, 1] * rows
    inside = jnp.minimum(jnp.maximum(departure_ref[row], low), high)
    return jnp.minimum(jnp.maximum(inside, 1), total_rows - 3)


def exchange_kernel(bands, levs, lat_t_ref, lon_t_ref, departure_ref, extents_ref, area_ref, fields_ref,
                    halo_ref, table_ref, held, mine, met, sent, gathered, send_sem, recv_sem, local_sem,
                    table_send_sem, table_recv_sem):
    band, lev = lax.axis_index("lat"), lax.axis_index("lev")
    group, position = band // 4, lax.rem(band, 4)
    groups = bands // 4
    has_up = group < groups - 1
    has_down = group > 0
    rows, field_count = fields_ref.shape[:2]
    first_row, total_rows = band * rows, bands * rows
    step_one = 1 - 2 * lax.rem(position, 2)
    step_two = 2 - 4 * (position // 2)
    across = [{"lev": 1 - lev}, {"lat": band + step_one}, {"lat": band + step_two}]
    others = [{"lat": lax.rem(band + 4 * j, bands)} for j in range(1, groups)]

    barrier = pltpu.get_barrier_semaphore()
    for peer in across + others:
        pl.semaphore_signal(barrier, inc=1, device_id=peer, device_id_type=MESH)
    pl.semaphore_wait(barrier, len(across) + len(others))

    def cut(part):
        first = field_count * part // 3
        return pl.ds(first, field_count * (part + 1) // 3 - first)

    def halo_part(distance, part):
        slot = distance + 4 if distance < 0 else distance + 3
        return halo_ref.at[pl.ds(slot * rows, rows), cut(part)]

    def when(offset, body):
        if offset == 0:
            body()
        else:
            pl.when(has_up if offset == 1 else has_down)(body)

    came_over = [
        {item: (link, k) for link, items in arrivals(member).items() for k, item in enumerate(items)}
        for member in range(4)
    ]
    waited = [set() for _ in range(4)]

    def wait_for(member, item):
        if item in waited[member]:
            return
        waited[member].add(item)
        offset, m, h = item
        link, k = came_over[member][item]
        place = halo_part(4 * offset + m - member, h)
        when(
            offset,
            lambda: pltpu.make_async_remote_copy(
                src_ref=place, dst_ref=place,
                send_sem=send_sem.at[LINKS.index(link), k],
                recv_sem=recv_sem.at[LINKS.index(link), k],
                device_id={"lat": band}, device_id_type=MESH,
            ).wait_recv(),
        )

    def targets(member):
        return [
            ("up", member, -4, -1),
            ("down", member, 4, 1),
            ("one", member ^ 1, (member ^ 1) - member, 0),
            ("two", member ^ 2, (member ^ 2) - member, 0),
        ]

    def sends(member, k):
        for link, target, step, group_step in targets(member):
            items = arrivals(target)[link]
            if k < len(items):
                offset, m, h = items[k]
                here = offset + group_step
                own = here == 0 and m == member
                copy = pltpu.make_async_remote_copy(
                    src_ref=fields_ref.at[:, cut(h)] if own else halo_part(4 * here + m - member, h),
                    dst_ref=halo_part(4 * offset + m - target, h),
                    send_sem=send_sem.at[LINKS.index(link), k],
                    recv_sem=recv_sem.at[LINKS.index(link), k],
                    device_id={"lat": band + step}, device_id_type=MESH,
                )
                yield (None if own else (here, m, h)), (group_step if group_step else here), copy

    def on_each(body):
        for member in range(4):
            pl.when(position == member)(functools.partial(body, member))

    def send_pieces(*steps):
        def body(member):
            for k in steps:
                for item, condition, copy in sends(member, k):
                    if item is not None:
                        wait_for(member, item)
                    when(condition, copy.start)

        on_each(body)

    def table_copy(n, source, target, peer):
        return pltpu.make_async_remote_copy(
            src_ref=source, dst_ref=target, send_sem=table_send_sem.at[n], recv_sem=table_recv_sem.at[n],
            device_id=peer, device_id_type=MESH,
        )

    load = pltpu.make_async_copy(fields_ref, held, local_sem)
    load.start()
    send_pieces(0)

    lane = lax.broadcasted_iota(jnp.int32, (1, table_ref.shape[1]), 1)
    taken = jnp.zeros(lane.shape, jnp.float32)
    for row in range(rows):
        departure = departure_of(row, first_row, rows, total_rows, departure_ref, extents_ref)
        lon_w = cubic(lon_t_ref[row])
        share = area_ref[first_row + row] * (lon_w[0] + lon_w[1] + lon_w[2] + lon_w[3]) * (1.0 / levs)
        for a, weight in enumerate(cubic(lat_t_ref[row])):
            taken = taken + jnp.where(lane == departure - 1 + a, share * weight, 0.0)
    load.wait()
    sums = [jnp.zeros(lane.shape, jnp.float32) for _ in range(field_count)]
    for row in range(rows):
        for f in range(field_count):
            total = jnp.sum(jnp.sum(held[row, f], axis=0, keepdims=True), axis=1, keepdims=True)
            sums[f] = sums[f] + jnp.where(lane == first_row + row, total, 0.0)
    mine[...] = jnp.zeros_like(mine)
    for f in range(field_count):
        mine[f:f + 1, :] = sums[f]
    mine[field_count:field_count + 1, :] = taken

    def table_step(n):
        return table_copy(n, mine if n == 0 else sent.at[n - 1], met.at[n], across[n])

    def table_add(n):
        table_step(n).wait_recv()
        sent[n] = (mine[...] if n == 0 else sent[n - 1]) + met[n]

    table_step(0).start()
    table_add(0)
    table_step(1).start()
    send_pieces(1, 2)
    table_add(1)
    table_step(2).start()
    send_pieces(3, 4)
    table_add(2)
    last = [table_copy(3 + j, sent.at[2], gathered.at[j], peer) for j, peer in enumerate(others)]
    for copy in last:
        copy.start()
    send_pieces(5, 6)
    for copy in last:
        copy.wait_recv()
    result = sent[2]
    for j in range(len(others)):
        result = result + gathered[j]
    table_ref[...] = result

    def finish(member):
        for k in range(7):
            for link in LINKS:
                items = arrivals(member)[link]
                if k < len(items):
                    wait_for(member, items[k])
        for k in range(7):
            for _, condition, copy in sends(member, k):
                when(condition, copy.wait_send)

    on_each(finish)
    for n in range(3):
        table_step(n).wait_send()
    for copy in last:
        copy.wait_send()


def exchange(lat_t, lon_t, departure_row, extents, area, fields):
    bands, levs = lax.axis_size("lat"), lax.axis_size("lev")
    rows, field_count = fields.shape[:2]
    table = ((field_count + 8) // 8 * 8, -(-bands * rows // LANES) * LANES)
    others = bands // 4 - 1
    return pl.pallas_call(
        functools.partial(exchange_kernel, bands, levs),
        out_shape=(
            jax.ShapeDtypeStruct((2 * REACH * rows,) + fields.shape[1:], fields.dtype),
            jax.ShapeDtypeStruct(table, jnp.float32),
        ),
        in_specs=[pl.BlockSpec(memory_space=pltpu.SMEM)] * 5 + [pl.BlockSpec(memory_space=pl.ANY)],
        out_specs=(pl.BlockSpec(memory_space=pl.ANY), pl.BlockSpec(memory_space=pltpu.VMEM)),
        scratch_shapes=[
            pltpu.VMEM(fields.shape, jnp.float32),
            pltpu.VMEM(table, jnp.float32),
            pltpu.VMEM((3,) + table, jnp.float32),
            pltpu.VMEM((3,) + table, jnp.float32),
            pltpu.VMEM((max(others, 1),) + table, jnp.float32),
            pltpu.SemaphoreType.DMA((4, 7)),
            pltpu.SemaphoreType.DMA((4, 7)),
            pltpu.SemaphoreType.DMA,
            pltpu.SemaphoreType.DMA((3 + others,)),
            pltpu.SemaphoreType.DMA((3 + others,)),
        ],
        compiler_params=pltpu.CompilerParams(collective_id=0, has_side_effects=True),
        name="exchange",
    )(lat_t, lon_t, departure_row, extents, area, fields)


def row_kernel(bands, lat_t_ref, lon_t_ref, shift_ref, departure_ref, extents_ref, table_ref, area_ref, fields_ref,
               halo_ref, out_ref, held, doubled, ratio, sem):
    row = pl.program_id(0)
    row_count = pl.num_programs(0)
    rows, field_count, _, lon_count = fields_ref.shape
    tiles = lon_count // LANES
    depth = held.shape[0]
    first_row = lax.axis_index("lat") * rows

    def fetch(index):
        slot = lax.rem(index, depth)
        departure = departure_of(index, first_row, rows, bands * rows, departure_ref, extents_ref)
        start = departure - 1 - (first_row - REACH * rows)
        low, high = REACH * rows, (REACH + 1) * rows
        outside = jnp.logical_or(start + 4 <= low, start >= high)

        @pl.when(outside)
        def _():
            away = jnp.where(start < low, start, start - rows)
            pltpu.make_async_copy(halo_ref.at[pl.ds(away, 4)], held.at[slot], sem.at[slot]).start()

        @pl.when(jnp.logical_not(outside))
        def _():
            for a in range(4):
                place = start + a
                own = jnp.logical_and(place >= low, place < high)
                target = held.at[slot, a]

                @pl.when(own)
                def _():
                    pltpu.make_async_copy(fields_ref.at[place - low], target, sem.at[slot]).start()

                @pl.when(jnp.logical_not(own))
                def _():
                    away = jnp.where(place < low, place, place - rows)
                    pltpu.make_async_copy(halo_ref.at[away], target, sem.at[slot]).start()

    @pl.when(row == 0)
    def _():
        for index in range(min(depth - 1, rows)):
            fetch(index)
        weight = table_ref[field_count:field_count + 1, :]
        for f in range(field_count):
            total = table_ref[f:f + 1, :]
            before = jnp.sum(total * area_ref[...], axis=1, keepdims=True)
            after = jnp.sum(total * weight, axis=1, keepdims=True)
            ratio[f] = jnp.broadcast_to(before / after, ratio.shape[1:])

    @pl.when(row + depth - 1 < row_count)
    def _():
        fetch(row + depth - 1)

    slot = lax.rem(row, depth)
    pltpu.make_async_copy(halo_ref.at[pl.ds(0, 4)], held.at[slot], sem.at[slot]).wait()
    lat_w, lon_w = cubic(lat_t_ref[row]), cubic(lon_t_ref[row])
    lane = lax.broadcasted_iota(jnp.int32, (out_ref.shape[2], LANES), 1)
    first = lax.rem(shift_ref[row] - 1 + lon_count, lon_count)
    whole, rest = first // LANES, lax.rem(first, LANES)
    turn = lax.rem(LANES - rest, LANES)
    keep = lane < LANES - rest

    def ahead(pieces, step):
        turned = [pltpu.roll(piece, LANES - step, 1) for piece in pieces]
        return [jnp.where(lane < LANES - step, turned[t], turned[(t + 1) % tiles]) for t in range(tiles)]

    for f in range(field_count):
        lon = [weight * ratio[f] for weight in lon_w]
        column = []
        for t in range(tiles):
            at = pl.ds(t * LANES, LANES)
            total = lat_w[0] * held[slot, 0, f, :, at]
            for a in range(1, 4):
                total = total + lat_w[a] * held[slot, a, f, :, at]
            column.append(total)
        after = ahead(column, 1)
        later = ahead([lon[2] * column[t] + lon[3] * after[t] for t in range(tiles)], 2)
        for t in range(tiles):
            mixed = lon[0] * column[t] + lon[1] * after[t] + later[t]
            doubled[f, :, t * LANES:(t + 1) * LANES] = mixed
            doubled[f, :, lon_count + t * LANES:lon_count + (t + 1) * LANES] = mixed
        turned = []
        for t in range(tiles + 1):
            at = pl.multiple_of((whole + t) * LANES, LANES)
            turned.append(pltpu.roll(doubled[f, :, pl.ds(at, LANES)], turn, 1))
        for t in range(tiles):
            out_ref[0, f, :, t * LANES:(t + 1) * LANES] = jnp.where(keep, turned[t], turned[t + 1])


def rows_of(bands, lat_t, lon_t, shift, departure_row, extents, table, area, fields, halo):
    rows, field_count, levels, lon_count = fields.shape
    smem = pl.BlockSpec(memory_space=pltpu.SMEM)
    return pl.pallas_call(
        functools.partial(row_kernel, bands),
        grid=(rows,),
        out_shape=jax.ShapeDtypeStruct(fields.shape, fields.dtype),
        in_specs=[smem] * 5 + [pl.BlockSpec(memory_space=pltpu.VMEM)] * 2 + [pl.BlockSpec(memory_space=pl.ANY)] * 2,
        out_specs=pl.BlockSpec((1, field_count, levels, lon_count), lambda r: (r, 0, 0, 0)),
        scratch_shapes=[
            pltpu.VMEM((DEPTH, 4, field_count, levels, lon_count), jnp.float32),
            pltpu.VMEM((field_count, levels, 2 * lon_count), jnp.float32),
            pltpu.VMEM((field_count, levels, LANES), jnp.float32),
            pltpu.SemaphoreType.DMA((DEPTH,)),
        ],
        compiler_params=pltpu.CompilerParams(dimension_semantics=("arbitrary",)),
        name="rows",
    )(lat_t, lon_t, shift, departure_row, extents, table, area, fields, halo)


def per_device(fields, lat_fraction, lon_fraction, lon_shift, departure_row, extents):
    bands = lax.axis_size("lat")
    total_rows = bands * fields.shape[0]
    row_ids = np.arange(-(-total_rows // LANES) * LANES)
    area = np.where(row_ids < total_rows, np.cos(math.pi * (row_ids + 0.5) / total_rows - math.pi / 2.0), 0.0)
    area = jnp.asarray(area, jnp.float32)
    halo, table = exchange(lat_fraction, lon_fraction, departure_row, extents, area, fields)
    return rows_of(
        bands, lat_fraction, lon_fraction, lon_shift, departure_row, extents, table, area[None, :], fields, halo
    )


def solution(mesh):
    return jax.shard_map(
        per_device,
        mesh=mesh,
        in_specs=(
            P("lat", None, "lev", None),
            P("lat"),
            P("lat"),
            P("lat"),
            P("lat"),
            P("lat", None),
        ),
        out_specs=P("lat", None, "lev", None),
        check_vma=False,
    )
```
